512 devices in a mesh: dp: 32 (over z_hi, x, core), seq: 16 (over z_lo, y).
Axes of the slice: x: 4, y: 8, z: 8 (z_hi: 4, z_lo: 2; z = z_hi * 2 + z_lo), core: 2. Of those that a mesh axis runs over, the one named last changes fastest.
Arguments:
- frames: bfloat16 [32, 2048, 1536], P('dp', 'seq'), may hold values from -8 to 8
- qkv_weight: bfloat16 [1536, 4608], P('dp'), may hold values from -2 to 2
- conv_kernel: bfloat16 [1536, 31], P('dp'), may hold values from -1 to 1
- lengths: int32 [32], P('dp'), may hold values from 1024 to 2048, as said below
Outputs:
- attended: bfloat16 [32, 2048, 1536], P('dp', 'seq')
- encoded: bfloat16 [32, 2048, 1536], P('dp', 'seq')
The draws below stay inside these ranges and needn't reach their ends.
Inputs may be any that keep to these rules, and one draw needn't show every extreme that they name: `lengths`: valid frames of each utterance; in every draw some utterance has exactly 2048.
All inputs are finite; a program needn't handle non-finite values.
Results may differ from the reference program's by a relative error of at most 0.0058.
Values may be sent and summed in bfloat16 or wider, within the bound.
No kernel may reach another device: no remote copies, remote signals or barrier semaphores. Data moves between devices by JAX's collectives and lax.ppermute only.
A program may use at most 64 MiB of HBM per device.

```python
import jax
import jax.numpy as jnp
from jax import lax

D = 1536
HEADS = 16
KERNEL = 31
HEAD_DIM = 96
LEN = 2048
UTT = 32


def draw_frames(key, part):
    first_key = jax.random.fold_in(key, 0)
    sample = jax.random.normal(first_key, (UTT, LEN, D), jnp.float32)
    return jnp.clip(sample, -8.0, 8.0).astype(jnp.bfloat16)


def draw_qkv_weight(key, part):
    first_key = jax.random.fold_in(key, 0)
    sample = jax.random.normal(first_key, (D, HEADS, 3, D // HEADS), jnp.float32) * D ** (-0.5)
    query_part = 2.0 * sample[:, :, 0]
    key_part = sample[:, :, 1]
    value_part = sample[:, :, 2]
    stacked = jnp.stack([query_part, key_part, value_part], axis=2)
    return jnp.clip(stacked.reshape(D, 3 * D), -2.0, 2.0).astype(jnp.bfloat16)


def draw_lengths(key, part):
    first_key, second_key = jax.random.split(key, 2)
    drawn = jax.random.randint(first_key, (UTT,), LEN // 2, LEN + 1)
    chosen = jax.random.randint(second_key, (), 0, UTT)
    return jnp.where(jnp.arange(UTT) == chosen, LEN, drawn).astype(jnp.int32)


def level_of(rng, extent, shards, smallest, high):
    loudness, own = 1.0, jax.random.fold_in(rng, 6)
    for dim, shards_of in shards:
        draws = jnp.exp(jax.random.uniform(jax.random.fold_in(own, dim), (shards_of,), jnp.float32, smallest / len(shards), high / len(shards)))
        loudness = loudness * jnp.repeat(draws, extent[dim] // shards_of).reshape([-1 if axis == dim else 1 for axis in range(len(extent))])
    return loudness


def bell_draw(key, dims, scale, most, cuts=(), kind=jnp.bfloat16):
    array = scale * jax.random.normal(key, dims, jnp.float32)
    if cuts:
        array = array * level_of(key, dims, cuts, -0.22, 0.18)
    return jnp.clip(array, -most, most).astype(kind)


def setup_inputs(seed: int = 0) -> dict:
    key_of = jax.random.split(jax.random.key(seed), 5)
    return {
        "frames": draw_frames(jax.random.fold_in(key_of[4], 71), 0),
        "qkv_weight": draw_qkv_weight(jax.random.fold_in(key_of[4], 71), 0),
        "conv_kernel": bell_draw(key_of[2], (D, KERNEL), KERNEL ** -0.5, 1.0, ((0, 32),)),
        "lengths": draw_lengths(jax.random.fold_in(key_of[4], 71), 0),
    }


EPSILON = 1e-05
NEG_BIG = -1e+30

def layer_norm(values):
    center = values - lax.optimization_barrier(jnp.mean(values, axis=-1, keepdims=True))
    return center * lax.rsqrt(lax.optimization_barrier(jnp.mean(center * center, axis=-1, keepdims=True)) + EPSILON)

def one_head(stacked, valid_rows):
    queries = stacked[:, :HEAD_DIM]
    keys_all = stacked[:, HEAD_DIM:2 * HEAD_DIM]
    values_all = stacked[:, 2 * HEAD_DIM:]
    scores = jnp.dot(queries, keys_all.T, preferred_element_type=jnp.float32) * HEAD_DIM ** (-0.5)
    scores = jnp.where(valid_rows[None, :], scores, NEG_BIG)
    highest = lax.optimization_barrier(jnp.max(scores, axis=1, keepdims=True))
    weights = jnp.exp(scores - highest)
    totals = lax.optimization_barrier(jnp.sum(weights, axis=1, keepdims=True))
    context = jnp.dot(weights.astype(jnp.bfloat16), values_all, preferred_element_type=jnp.float32) / totals
    return context.astype(jnp.bfloat16)

def reference(frames, qkv_weight, conv_kernel, lengths):
    kernel_wide = conv_kernel.astype(jnp.float32)
    reach = (KERNEL - 1) // 2

    def utterance(inputs):
        one_frames, length = inputs
        valid_rows = jnp.arange(LEN, dtype=jnp.int32) < length
        inputs_wide = one_frames.astype(jnp.float32)
        normed = layer_norm(inputs_wide).astype(jnp.bfloat16)
        projected = jnp.dot(normed, qkv_weight, preferred_element_type=jnp.float32).astype(jnp.bfloat16)
        projected = projected.reshape(LEN, HEADS, 3 * HEAD_DIM).transpose(1, 0, 2)
        context = lax.map(lambda stacked: one_head(stacked, valid_rows), projected)
        context = context.transpose(1, 0, 2).reshape(LEN, D)
        attended = jnp.where(valid_rows[:, None], inputs_wide + context.astype(jnp.float32), 0.0).astype(jnp.bfloat16)
        conv_input = jnp.where(valid_rows[:, None], layer_norm(attended.astype(jnp.float32)), 0.0).astype(jnp.bfloat16)
        padded = jnp.pad(conv_input, ((reach, reach), (0, 0)))
        mixture = jnp.zeros((LEN, D), jnp.float32)
        for tap_index in range(KERNEL):
            mixture = mixture + padded[tap_index:tap_index + LEN].astype(jnp.float32) * kernel_wide[:, tap_index]
        encoded = jnp.where(valid_rows[:, None], attended.astype(jnp.float32) + jax.nn.silu(mixture), 0.0)
        return (attended, encoded.astype(jnp.bfloat16))
    attended, encoded = lax.map(utterance, (frames, lengths))
    return (attended, encoded)
```

```python
import functools

import jax
import jax.numpy as jnp
from jax import lax
from jax.experimental import pallas as pl
from jax.experimental.pallas import tpu as pltpu
from jax.sharding import Mesh
from jax.sharding import PartitionSpec as P

HEADS = 16
KERNEL = 31
HEAD_DIM = 96
EPSILON = 1e-05
NEG_BIG = -1e30

LANES = 128
ROWS = 128
RING = 8
HALO = 16
WINDOW = ROWS + 2 * HALO
GROUPS = 4
GROUP_ROWS = WINDOW // GROUPS
STRIDE = 3 * HEAD_DIM
PIECE = 640
PADDED = 3 * LANES
TAPS_AT = 2 * STRIDE
Q_ROWS = 256
K_ROWS = 512

VMEM = pl.BlockSpec(memory_space=pltpu.VMEM)
SMEM = pl.BlockSpec(memory_space=pltpu.SMEM)
F32 = jnp.float32
BF16 = jnp.bfloat16


def call(kernel, outs, scalars, *arrays, scratch=()):
    return pl.pallas_call(
        kernel,
        out_shape=outs,
        in_specs=[SMEM] + [VMEM] * len(arrays),
        out_specs=jax.tree.map(lambda _: VMEM, outs),
        scratch_shapes=list(scratch),
        compiler_params=pltpu.CompilerParams(vmem_limit_bytes=40 * 2**20),
    )(scalars, *arrays)


def normalized(values):
    center = values - jnp.mean(values, axis=-1, keepdims=True)
    return center * lax.rsqrt(jnp.mean(center * center, axis=-1, keepdims=True) + EPSILON)


def assemble_kernel(scalars, own, x1, x2, x3, other, weight, taps, gathered):
    place = scalars[0]
    rows = 48
    for core in range(2):
        for x in range(4):
            source = (own, x1, x2, x3)[x] if core == 0 else other
            base = 0 if core == 0 else x * 4 * rows
            for z in range(4):
                target = pl.multiple_of(((z * 8 + x * 2 + core) ^ place) * rows, 16)
                gathered[pl.ds(target, rows), :] = source[base + z * rows : base + (z + 1) * rows, :]
    first = TAPS_AT - (PIECE - LANES)
    blank = jnp.zeros((LANES, LANES - HEAD_DIM), F32)
    for tile in range(12):
        span = slice(tile * LANES, (tile + 1) * LANES)
        piece = gathered[span, :].astype(F32)
        for part in range(6):
            columns = piece[:, part * HEAD_DIM : (part + 1) * HEAD_DIM]
            weight[span, part * LANES : (part + 1) * LANES] = jnp.concatenate(
                [columns, blank], axis=1
            ).astype(BF16)
        taps[:, span] = piece[:, PIECE - LANES :].T[first : first + 32, :]


def project_kernel(scalars, weight, *refs):
    blocks, (mine, theirs) = refs[:-2], refs[-2:]
    at = 0
    for block in blocks:
        rows = block.shape[0]
        normed = normalized(block[...].astype(F32)).astype(BF16)
        result = jnp.dot(normed, weight[...], preferred_element_type=F32).astype(BF16)
        mine[at : at + rows, :] = result[:, :PADDED]
        theirs[at : at + rows, :] = result[:, PADDED:]
        at += rows


def attention_kernel(scalars, *refs):
    chunks, out = refs[:8], refs[8]
    queries, keys, values, context = refs[9:]
    y, half, length = scalars[1], scalars[2], scalars[3]
    sign = 1 - 2 * (y % 2)
    lane = lax.broadcasted_iota(jnp.int32, (ROWS, LANES), 1)
    row = lax.broadcasted_iota(jnp.int32, (ROWS, LANES), 0)
    steps = ((0, 1, -1), (2, -2), (3, -3), (4,))
    for side in range(2):
        for group in range(4):
            chunk = chunks[side * 4 + group]
            for index, step in enumerate(steps[group]):
                source = (y + sign * step + RING) % RING
                which = half if side == 0 else 1 - half
                start = pl.multiple_of((which * RING + source) * ROWS, ROWS)
                span = slice(index * ROWS, (index + 1) * ROWS)
                to = pl.ds(start, ROWS)
                queries[to, :] = jnp.where(
                    lane == HEAD_DIM, 1.0, chunk[span, :LANES].astype(F32)
                ).astype(BF16)
                masked = jnp.where(start + row < length, 0.0, NEG_BIG)
                keys[to, :] = jnp.where(
                    lane == HEAD_DIM, masked, chunk[span, LANES : 2 * LANES].astype(F32)
                ).astype(BF16)
                values[to, :] = jnp.where(
                    lane == HEAD_DIM, 1.0, chunk[span, 2 * LANES :].astype(F32)
                ).astype(BF16)
    total = queries.shape[0]
    factor = HEAD_DIM**-0.5 * 1.4426950408889634
    context[:HALO, :] = jnp.zeros((HALO, LANES), BF16)
    context[HALO + total :, :] = jnp.zeros((HALO, LANES), BF16)

    def visit(index, _):
        first = pl.multiple_of(index * Q_ROWS, Q_ROWS)
        query = queries[pl.ds(first, Q_ROWS), :]
        highest = jnp.full((Q_ROWS, 1), NEG_BIG, F32)
        summed = jnp.zeros((Q_ROWS, LANES), F32)
        for block in range(total // K_ROWS):
            part = slice(block * K_ROWS, (block + 1) * K_ROWS)
            scores = lax.dot_general(
                query, keys[part, :], (((1,), (1,)), ((), ())), preferred_element_type=F32
            )
            raised = jnp.maximum(highest, jnp.max(scores, axis=1, keepdims=True))
            weights = jnp.exp2((scores - raised) * factor).astype(BF16)
            shrink = jnp.exp2((highest - raised) * factor)
            summed = summed * shrink + jnp.dot(
                weights, values[part, :], preferred_element_type=F32
            )
            highest = raised
        context[pl.ds(HALO + first, Q_ROWS), :] = (
            summed / summed[:, HEAD_DIM : HEAD_DIM + 1]
        ).astype(BF16)
        return 0

    lax.fori_loop(0, total // Q_ROWS, visit, 0)
    for target in range(total // ROWS):
        parts = [
            context[
                target * ROWS + group * GROUP_ROWS : target * ROWS + (group + 1) * GROUP_ROWS,
                :HEAD_DIM,
            ]
            for group in range(GROUPS)
        ]
        out[target] = jnp.concatenate(parts, axis=1)


def finish_kernel(scalars, returned, own, low, high, taps, attended, encoded, wide):
    begin, length = scalars[4], scalars[3]
    rows = []
    for group in range(GROUPS):
        span = slice(group * HEAD_DIM, (group + 1) * HEAD_DIM)
        rows.append(
            jnp.concatenate([returned[head, :, span] for head in range(HEADS)], axis=1)
        )
    context = jnp.concatenate(rows, axis=0).astype(F32)
    inputs = jnp.concatenate([low[...], own[...], high[...]], axis=0).astype(F32)
    position = begin - HALO + lax.broadcasted_iota(jnp.int32, (WINDOW, 1), 0)
    valid = jnp.logical_and(position >= 0, position < length)
    summed = jnp.where(valid, inputs + context, 0.0).astype(BF16)
    attended[...] = summed[HALO : HALO + ROWS, :]
    conv_input = jnp.where(valid, normalized(summed.astype(F32)), 0.0).astype(BF16).astype(F32)
    tiles = wide.shape[0]
    for tile in range(tiles):
        wide[tile] = conv_input[:, tile * LANES : (tile + 1) * LANES]
    kept = valid[HALO : HALO + ROWS]
    for tile in range(tiles):
        span = slice(tile * LANES, (tile + 1) * LANES)
        mixture = jnp.zeros((ROWS, LANES), F32)
        for tap in range(KERNEL):
            at = tap + HALO - KERNEL // 2
            mixture = mixture + wide[tile, at : at + ROWS, :] * taps[tap : tap + 1, span]
        active = mixture / (1.0 + jnp.exp(-mixture))
        encoded[:, span] = jnp.where(
            kept, attended[:, span].astype(F32) + active, 0.0
        ).astype(BF16)


def xor_pairs(count, by):
    return [(i, i ^ by) for i in range(count)]


def on_device(frames, qkv_weight, conv_kernel, lengths):
    own = frames[0]
    place_y, half = lax.axis_index("y"), lax.axis_index("zl")
    place = lax.axis_index(("zh", "x", "c"))
    sequence = half * RING + place_y
    scalars = jnp.stack([place, place_y, half, lengths[0], sequence * ROWS]).astype(jnp.int32)

    one = xor_pairs(RING, 1)
    two = [(i, (i - 1 if i % 2 == 0 else i + 1) % RING) for i in range(RING)]

    def swap_one(block):
        return lax.ppermute(block, "y", one)

    def swap_two(block):
        return lax.ppermute(block, "y", two)

    columns = [
        lax.dynamic_slice_in_dim(qkv_weight, (which * RING + place_y) * STRIDE, STRIDE, 1)
        for which in (half, 1 - half)
    ]
    piece = jnp.concatenate(
        columns + [conv_kernel, jnp.zeros((48, PIECE - 2 * STRIDE - KERNEL), BF16)], axis=1
    )
    a1, b1 = swap_one(own), swap_two(own)
    piece = jnp.concatenate(
        [piece] + [lax.ppermute(piece, "zh", xor_pairs(4, by)) for by in (1, 2, 3)], axis=0
    )
    a2, b2 = swap_one(b1), swap_two(a1)
    across = [lax.ppermute(piece, "x", xor_pairs(4, by)) for by in (1, 2, 3)]
    other = lax.ppermute(jnp.concatenate([piece] + across, axis=0), "c", xor_pairs(2, 1))
    a3, b3 = swap_one(b2), swap_two(a2)
    a4, b4 = swap_one(b3[: ROWS // 2]), swap_two(a3[ROWS // 2 :])

    edge = lax.ppermute(
        jnp.where(half == 0, own[ROWS - HALO :], own[:HALO]),
        ("zl", "y"),
        [(RING - 1, RING), (RING, RING - 1)],
    )
    even = place_y % 2 == 0
    low = jnp.where(even, b1[ROWS - HALO :], a1[ROWS - HALO :])
    high = jnp.where(even, a1[:HALO], b1[:HALO])
    low = jnp.where(place_y == 0, edge, low)
    high = jnp.where(place_y == RING - 1, edge, high)

    weight, taps = call(
        assemble_kernel,
        (
            jax.ShapeDtypeStruct((1536, 2 * PADDED), BF16),
            jax.ShapeDtypeStruct((32, 1536), F32),
        ),
        scalars,
        piece,
        *across,
        other,
        scratch=[pltpu.VMEM((1536, PIECE), BF16)],
    )
    mine, theirs = [], []
    for blocks in ((own, a1, b1), (a2, b2), (a3, b3), (a4, b4)):
        shape = jax.ShapeDtypeStruct((sum(b.shape[0] for b in blocks), PADDED), BF16)
        kept, sent = call(project_kernel, (shape, shape), scalars, weight, *blocks)
        mine.append(kept)
        theirs.append(lax.ppermute(sent, "zl", xor_pairs(2, 1)))
    context = call(
        attention_kernel,
        jax.ShapeDtypeStruct((HEADS, GROUP_ROWS, GROUPS * HEAD_DIM), BF16),
        scalars,
        *mine,
        *theirs,
        scratch=[
            pltpu.VMEM((2 * RING * ROWS, LANES), BF16),
            pltpu.VMEM((2 * RING * ROWS, LANES), BF16),
            pltpu.VMEM((2 * RING * ROWS, LANES), BF16),
            pltpu.VMEM((2 * RING * ROWS + 2 * HALO, LANES), BF16),
        ],
    )
    returned = lax.all_to_all(context, ("zl", "y"), split_axis=0, concat_axis=0, tiled=True)
    shape = jax.ShapeDtypeStruct(own.shape, BF16)
    attended, encoded = call(
        finish_kernel,
        (shape, shape),
        scalars,
        returned,
        own,
        low,
        high,
        taps,
        scratch=[pltpu.VMEM((1536 // LANES, WINDOW, LANES), F32)],
    )
    return attended[None], encoded[None]


def solution(mesh):
    fine = Mesh(mesh.devices.reshape(4, 4, 2, 2, RING), ("zh", "x", "c", "zl", "y"))
    rows, columns = ("zh", "x", "c"), ("zl", "y")
    in_specs = (P(rows, columns, None), P(rows, None), P(rows, None), P(rows))
    out_specs = (P(rows, columns, None), P(rows, columns, None))
    return jax.shard_map(
        on_device, mesh=fine, in_specs=in_specs, out_specs=out_specs, check_vma=False
    )
```

```python
import jax
import jax.numpy as jnp
from jax import lax
from jax.experimental import pallas as pl
from jax.experimental.pallas import tpu as pltpu
from jax.sharding import Mesh
from jax.sharding import PartitionSpec as P


HEADS = 16
KERNEL = 31
HEAD_DIM = 96
EPSILON = 1e-05
NEG_BIG = -1e30

LANES = 128
ROWS = 128
RING = 8
HALO = 16
WINDOW = ROWS + 2 * HALO
GROUPS = 4
GROUP_ROWS = WINDOW // GROUPS
STRIDE = 3 * HEAD_DIM
PIECE = 640
PADDED = 3 * LANES
TAPS_AT = 2 * STRIDE
Q_ROWS = 256
K_ROWS = 512

VMEM = pl.BlockSpec(memory_space=pltpu.VMEM)
SMEM = pl.BlockSpec(memory_space=pltpu.SMEM)
F32 = jnp.float32
BF16 = jnp.bfloat16


def call(kernel, outs, scalars, *arrays, scratch=()):
    return pl.pallas_call(
        kernel,
        out_shape=outs,
        in_specs=[SMEM] + [VMEM] * len(arrays),
        out_specs=jax.tree.map(lambda _: VMEM, outs),
        scratch_shapes=list(scratch),
        compiler_params=pltpu.CompilerParams(vmem_limit_bytes=40 * 2**20),
    )(scalars, *arrays)


def normalized(values):
    center = values - jnp.mean(values, axis=-1, keepdims=True)
    return center * lax.rsqrt(jnp.mean(center * center, axis=-1, keepdims=True) + EPSILON)


def assemble_kernel(scalars, own, other, weight, taps, gathered):
    core = scalars[0] % 2
    rows = 48
    for source, which in ((own, core), (other, 1 - core)):
        for x in range(4):
            for z in range(4):
                target = pl.multiple_of((z * 8 + x * 2 + which) * rows, 16)
                at = (x * 4 + z) * rows
                gathered[pl.ds(target, rows), :] = source[at : at + rows, :]
    first = TAPS_AT - (PIECE - LANES)
    blank = jnp.zeros((LANES, LANES - HEAD_DIM), F32)
    for tile in range(12):
        span = slice(tile * LANES, (tile + 1) * LANES)
        piece = gathered[span, :].astype(F32)
        for part in range(6):
            columns = piece[:, part * HEAD_DIM : (part + 1) * HEAD_DIM]
            weight[span, part * LANES : (part + 1) * LANES] = jnp.concatenate(
                [columns, blank], axis=1
            ).astype(BF16)
        taps[:, span] = piece[:, PIECE - LANES :].T[first : first + 32, :]


def project_kernel(scalars, weight, *refs):
    blocks, (mine, theirs) = refs[:-2], refs[-2:]
    at = 0
    for block in blocks:
        rows = block.shape[0]
        normed = normalized(block[...].astype(F32)).astype(BF16)
        result = jnp.dot(normed, weight[...], preferred_element_type=F32).astype(BF16)
        mine[at : at + rows, :] = result[:, :PADDED]
        theirs[at : at + rows, :] = result[:, PADDED:]
        at += rows


def attention_kernel(scalars, *refs):
    chunks, out = refs[:8], refs[8]
    queries, keys, values, context = refs[9:]
    y, half, length = scalars[1], scalars[2], scalars[3]
    sign = 1 - 2 * (y % 2)
    lane = lax.broadcasted_iota(jnp.int32, (ROWS, LANES), 1)
    row = lax.broadcasted_iota(jnp.int32, (ROWS, LANES), 0)
    steps = ((0, 1, -1), (2, -2), (3, -3), (4,))
    for side in range(2):
        for group in range(4):
            chunk = chunks[side * 4 + group]
            for index, step in enumerate(steps[group]):
                source = (y + sign * step + RING) % RING
                which = half if side == 0 else 1 - half
                start = pl.multiple_of((which * RING + source) * ROWS, ROWS)
                span = slice(index * ROWS, (index + 1) * ROWS)
                to = pl.ds(start, ROWS)
                queries[to, :] = jnp.where(
                    lane == HEAD_DIM, 1.0, chunk[span, :LANES].astype(F32)
                ).astype(BF16)
                masked = jnp.where(start + row < length, 0.0, NEG_BIG)
                keys[to, :] = jnp.where(
                    lane == HEAD_DIM, masked, chunk[span, LANES : 2 * LANES].astype(F32)
                ).astype(BF16)
                values[to, :] = jnp.where(
                    lane == HEAD_DIM, 1.0, chunk[span, 2 * LANES :].astype(F32)
                ).astype(BF16)
    total = queries.shape[0]
    factor = HEAD_DIM**-0.5 * 1.4426950408889634
    context[:HALO, :] = jnp.zeros((HALO, LANES), BF16)
    context[HALO + total :, :] = jnp.zeros((HALO, LANES), BF16)

    def visit(index, _):
        first = pl.multiple_of(index * Q_ROWS, Q_ROWS)
        query = queries[pl.ds(first, Q_ROWS), :]
        highest = jnp.full((Q_ROWS, 1), NEG_BIG, F32)
        summed = jnp.zeros((Q_ROWS, LANES), F32)
        for block in range(total // K_ROWS):
            part = slice(block * K_ROWS, (block + 1) * K_ROWS)
            scores = lax.dot_general(
                query, keys[part, :], (((1,), (1,)), ((), ())), preferred_element_type=F32
            )
            raised = jnp.maximum(highest, jnp.max(scores, axis=1, keepdims=True))
            weights = jnp.exp2((scores - raised) * factor).astype(BF16)
            shrink = jnp.exp2((highest - raised) * factor)
            summed = summed * shrink + jnp.dot(
                weights, values[part, :], preferred_element_type=F32
            )
            highest = raised
        context[pl.ds(HALO + first, Q_ROWS), :] = (
            summed / summed[:, HEAD_DIM : HEAD_DIM + 1]
        ).astype(BF16)
        return 0

    lax.fori_loop(0, total // Q_ROWS, visit, 0)
    for target in range(total // ROWS):
        parts = [
            context[
                target * ROWS + group * GROUP_ROWS : target * ROWS + (group + 1) * GROUP_ROWS,
                :HEAD_DIM,
            ]
            for group in range(GROUPS)
        ]
        out[target] = jnp.concatenate(parts, axis=1)


def finish_kernel(scalars, returned, own, low, high, taps, attended, encoded, wide):
    begin, length = scalars[4], scalars[3]
    rows = []
    for group in range(GROUPS):
        span = slice(group * HEAD_DIM, (group + 1) * HEAD_DIM)
        rows.append(
            jnp.concatenate([returned[head, :, span] for head in range(HEADS)], axis=1)
        )
    context = jnp.concatenate(rows, axis=0).astype(F32)
    inputs = jnp.concatenate([low[...], own[...], high[...]], axis=0).astype(F32)
    position = begin - HALO + lax.broadcasted_iota(jnp.int32, (WINDOW, 1), 0)
    valid = jnp.logical_and(position >= 0, position < length)
    summed = jnp.where(valid, inputs + context, 0.0).astype(BF16)
    attended[...] = summed[HALO : HALO + ROWS, :]
    conv_input = jnp.where(valid, normalized(summed.astype(F32)), 0.0).astype(BF16).astype(F32)
    tiles = wide.shape[0]
    for tile in range(tiles):
        wide[tile] = conv_input[:, tile * LANES : (tile + 1) * LANES]
    kept = valid[HALO : HALO + ROWS]
    for tile in range(tiles):
        span = slice(tile * LANES, (tile + 1) * LANES)
        mixture = jnp.zeros((ROWS, LANES), F32)
        for tap in range(KERNEL):
            at = tap + HALO - KERNEL // 2
            mixture = mixture + wide[tile, at : at + ROWS, :] * taps[tap : tap + 1, span]
        active = mixture / (1.0 + jnp.exp(-mixture))
        encoded[:, span] = jnp.where(
            kept, attended[:, span].astype(F32) + active, 0.0
        ).astype(BF16)


def xor_pairs(count, by):
    return [(i, i ^ by) for i in range(count)]


def on_device(frames, qkv_weight, conv_kernel, lengths):
    own = frames[0]
    place_y, half = lax.axis_index("y"), lax.axis_index("zl")
    place = lax.axis_index(("zh", "x", "c"))
    sequence = half * RING + place_y
    scalars = jnp.stack([place, place_y, half, lengths[0], sequence * ROWS]).astype(jnp.int32)

    one = xor_pairs(RING, 1)
    two = [(i, (i - 1 if i % 2 == 0 else i + 1) % RING) for i in range(RING)]

    def spread(block, axis):
        copies = jnp.broadcast_to(block[None], (4, *block.shape))
        filled = lax.all_to_all(copies, axis, split_axis=0, concat_axis=0, tiled=True)
        return filled.reshape(-1, block.shape[1])

    a1, b1 = lax.ppermute(own, "y", one), lax.ppermute(own, "y", two)
    a2, b2 = lax.ppermute(b1, "y", one), lax.ppermute(a1, "y", two)
    a3, b3 = lax.ppermute(b2, "y", one), lax.ppermute(a2, "y", two)
    a4 = lax.ppermute(b3[: ROWS // 2], "y", one)
    b4 = lax.ppermute(a3[ROWS // 2 :], "y", two)

    columns = [
        lax.dynamic_slice_in_dim(qkv_weight, (which * RING + place_y) * STRIDE, STRIDE, 1)
        for which in (half, 1 - half)
    ]
    piece = jnp.concatenate(
        columns + [conv_kernel, jnp.zeros((48, PIECE - 2 * STRIDE - KERNEL), BF16)], axis=1
    )
    gathered = spread(spread(piece, "zh"), "x")
    other = lax.ppermute(gathered, "c", xor_pairs(2, 1))

    edge = lax.ppermute(
        jnp.where(half == 0, own[ROWS - HALO :], own[:HALO]),
        ("zl", "y"),
        [(RING - 1, RING), (RING, RING - 1)],
    )
    even = place_y % 2 == 0
    low = jnp.where(even, b1[ROWS - HALO :], a1[ROWS - HALO :])
    high = jnp.where(even, a1[:HALO], b1[:HALO])
    low = jnp.where(place_y == 0, edge, low)
    high = jnp.where(place_y == RING - 1, edge, high)

    weight, taps = call(
        assemble_kernel,
        (
            jax.ShapeDtypeStruct((1536, 2 * PADDED), BF16),
            jax.ShapeDtypeStruct((32, 1536), F32),
        ),
        scalars,
        gathered,
        other,
        scratch=[pltpu.VMEM((1536, PIECE), BF16)],
    )
    mine, theirs = [], []
    for blocks in ((own, a1, b1), (a2, b2), (a3, b3), (a4, b4)):
        shape = jax.ShapeDtypeStruct((sum(b.shape[0] for b in blocks), PADDED), BF16)
        kept, sent = call(project_kernel, (shape, shape), scalars, weight, *blocks)
        mine.append(kept)
        theirs.append(lax.ppermute(sent, "zl", xor_pairs(2, 1)))
    context = call(
        attention_kernel,
        jax.ShapeDtypeStruct((HEADS, GROUP_ROWS, GROUPS * HEAD_DIM), BF16),
        scalars,
        *mine,
        *theirs,
        scratch=[
            pltpu.VMEM((2 * RING * ROWS, LANES), BF16),
            pltpu.VMEM((2 * RING * ROWS, LANES), BF16),
            pltpu.VMEM((2 * RING * ROWS, LANES), BF16),
            pltpu.VMEM((2 * RING * ROWS + 2 * HALO, LANES), BF16),
        ],
    )
    returned = lax.all_to_all(context, ("zl", "y"), split_axis=0, concat_axis=0, tiled=True)
    shape = jax.ShapeDtypeStruct(own.shape, BF16)
    attended, encoded = call(
        finish_kernel,
        (shape, shape),
        scalars,
        returned,
        own,
        low,
        high,
        taps,
        scratch=[pltpu.VMEM((1536 // LANES, WINDOW, LANES), F32)],
    )
    return attended[None], encoded[None]


def solution(mesh):
    fine = Mesh(mesh.devices.reshape(4, 4, 2, 2, RING), ("zh", "x", "c", "zl", "y"))
    rows, columns = ("zh", "x", "c"), ("zl", "y")
    in_specs = (P(rows, columns, None), P(rows, None), P(rows, None), P(rows))
    out_specs = (P(rows, columns, None), P(rows, columns, None))

    return jax.shard_map(
        on_device, mesh=fine, in_specs=in_specs, out_specs=out_specs, check_vma=False
    )
```

```python
import functools

import jax
import jax.numpy as jnp
from jax import lax
from jax.experimental import pallas as pl
from jax.experimental.pallas import tpu as pltpu
from jax.sharding import Mesh
from jax.sharding import PartitionSpec as P


HEADS = 16
KERNEL = 31
HEAD_DIM = 96
EPSILON = 1e-05
NEG_BIG = -1e30

LANES = 128
ROWS = 128
RING = 8
HALO = 16
WINDOW = ROWS + 2 * HALO
GROUPS = 4
GROUP_ROWS = WINDOW // GROUPS
STRIDE = 3 * HEAD_DIM
PIECE = 640
TAPS_AT = 2 * STRIDE
PACK = 4
PACKED = (ROWS // PACK, PACK * STRIDE)
CHUNKS = ((0, 1, -1, 2, -2), (3, -3), (4,))
Q_ROWS = 256
K_ROWS = 2048

VMEM = pl.BlockSpec(memory_space=pltpu.VMEM)
SMEM = pl.BlockSpec(memory_space=pltpu.SMEM)
F32 = jnp.float32
BF16 = jnp.bfloat16


def call(kernel, outs, scalars, *arrays, scratch=()):
    return pl.pallas_call(
        kernel,
        out_shape=outs,
        in_specs=[SMEM] + [VMEM] * len(arrays),
        out_specs=jax.tree.map(lambda _: VMEM, outs),
        scratch_shapes=list(scratch),
        compiler_params=pltpu.CompilerParams(vmem_limit_bytes=16 * 2**20),
    )(scalars, *arrays)


def normalized(values):
    center = values - jnp.mean(values, axis=-1, keepdims=True)
    return center * lax.rsqrt(jnp.mean(center * center, axis=-1, keepdims=True) + EPSILON)


def project(blocks, weight, mine, theirs, normed):
    at = 0
    for block in blocks:
        rows = block.shape[0]
        normed[at : at + rows, :] = normalized(block[...].astype(F32)).astype(BF16)
        at += rows
    result = jnp.dot(normed[...], weight[...], preferred_element_type=F32)
    rows, _ = PACKED
    for block in range(at // ROWS):
        for head, target in enumerate((mine, theirs)):
            parts = []
            for group in range(PACK):
                first = block * ROWS + group * rows
                parts.append(
                    result[first : first + rows, head * STRIDE : (head + 1) * STRIDE]
                )
            target[block * rows : (block + 1) * rows, :] = jnp.concatenate(
                parts, axis=1
            ).astype(BF16)


def first_kernel(scalars, own, other, *refs):
    *blocks, weight, mine, theirs, normed = refs
    core = scalars[0] % 2
    rows = 48
    for source, which in ((own, core), (other, 1 - core)):
        for x in range(4):
            for z in range(4):
                target = pl.multiple_of((z * 8 + x * 2 + which) * rows, 16)
                at = (x * 4 + z) * rows
                weight[pl.ds(target, rows), :] = source[at : at + rows, :]
    project(blocks, weight, mine, theirs, normed)


def second_kernel(scalars, weight, *refs):
    *blocks, taps, mine, theirs, normed = refs
    first = TAPS_AT - (PIECE - LANES)
    for tile in range(1536 // LANES):
        span = slice(tile * LANES, (tile + 1) * LANES)
        taps[:, span] = weight[span, PIECE - LANES :].astype(F32).T[first : first + 32, :]
    project(blocks, weight, mine, theirs, normed)


def project_kernel(scalars, weight, *refs):
    *blocks, mine, theirs, normed = refs
    project(blocks, weight, mine, theirs, normed)


def attention_kernel(scalars, *refs):
    groups = len(CHUNKS)
    chunks, out = refs[: 2 * groups], refs[2 * groups]
    queries, keys, values, context = refs[2 * groups + 1 :]
    y, half, length = scalars[1], scalars[2], scalars[3]
    sign = 1 - 2 * (y % 2)
    rows = ROWS // PACK
    row = lax.broadcasted_iota(jnp.int32, (rows, LANES), 0)
    blank = jnp.zeros((rows, LANES - HEAD_DIM), F32)
    marked = lax.broadcasted_iota(jnp.int32, (rows, LANES), 1) == HEAD_DIM
    for side in range(2):
        for group, steps in enumerate(CHUNKS):
            chunk = chunks[side * groups + group]
            for index, step in enumerate(steps):
                source = (y + sign * step + RING) % RING
                which = half if side == 0 else 1 - half
                packed = chunk[index * rows : (index + 1) * rows, :].astype(F32)
                for part in range(PACK):
                    start = (which * RING + source) * ROWS + part * rows
                    to = pl.ds(pl.multiple_of(start, rows), rows)
                    ends = (1.0, jnp.where(start + row < length, 0.0, NEG_BIG), 1.0)
                    for kind, target in enumerate((queries, keys, values)):
                        first = part * STRIDE + kind * HEAD_DIM
                        columns = packed[:, first : first + HEAD_DIM]
                        columns = jnp.concatenate([columns, blank], axis=1)
                        target[to, :] = jnp.where(marked, ends[kind], columns).astype(BF16)
    total = queries.shape[0]
    factor = HEAD_DIM**-0.5 * 1.4426950408889634
    context[:HALO, :] = jnp.zeros((HALO, LANES), BF16)
    context[HALO + total :, :] = jnp.zeros((HALO, LANES), BF16)

    def visit(index, _):
        first = pl.multiple_of(index * Q_ROWS, Q_ROWS)
        query = queries[pl.ds(first, Q_ROWS), :]
        parts = [slice(b * K_ROWS, (b + 1) * K_ROWS) for b in range(total // K_ROWS)]
        scores = [
            lax.dot_general(
                query, keys[part, :], (((1,), (1,)), ((), ())), preferred_element_type=F32
            )
            for part in parts
        ]
        highest = functools.reduce(
            jnp.maximum, [jnp.max(block, axis=1, keepdims=True) for block in scores]
        )
        summed = jnp.zeros((Q_ROWS, LANES), F32)
        for block, part in zip(scores, parts):
            weights = jnp.exp2((block - highest) * factor).astype(BF16)
            summed += jnp.dot(weights, values[part, :], preferred_element_type=F32)
        context[pl.ds(HALO + first, Q_ROWS), :] = (
            summed / summed[:, HEAD_DIM : HEAD_DIM + 1]
        ).astype(BF16)
        return 0

    lax.fori_loop(0, total // Q_ROWS, visit, 0, unroll=2)
    for target in range(total // ROWS):
        parts = [
            context[
                target * ROWS + group * GROUP_ROWS : target * ROWS + (group + 1) * GROUP_ROWS,
                :HEAD_DIM,
            ]
            for group in range(GROUPS)
        ]
        out[target] = jnp.concatenate(parts, axis=1)


def finish_kernel(scalars, returned, own, low, high, taps, attended, encoded, wide):
    begin, length = scalars[4], scalars[3]
    rows = []
    for group in range(GROUPS):
        span = slice(group * HEAD_DIM, (group + 1) * HEAD_DIM)
        rows.append(
            jnp.concatenate([returned[head, :, span] for head in range(HEADS)], axis=1)
        )
    context = jnp.concatenate(rows, axis=0).astype(F32)
    inputs = jnp.concatenate([low[...], own[...], high[...]], axis=0).astype(F32)
    position = begin - HALO + lax.broadcasted_iota(jnp.int32, (WINDOW, 1), 0)
    valid = jnp.logical_and(position >= 0, position < length)
    summed = jnp.where(valid, inputs + context, 0.0).astype(BF16)
    attended[...] = summed[HALO : HALO + ROWS, :]
    conv_input = jnp.where(valid, normalized(summed.astype(F32)), 0.0).astype(BF16).astype(F32)
    tiles = wide.shape[0]
    for tile in range(tiles):
        wide[tile] = conv_input[:, tile * LANES : (tile + 1) * LANES]
    kept = valid[HALO : HALO + ROWS]
    for tile in range(tiles):
        span = slice(tile * LANES, (tile + 1) * LANES)
        mixture = jnp.zeros((ROWS, LANES), F32)
        for tap in range(KERNEL):
            at = tap + HALO - KERNEL // 2
            mixture = mixture + wide[tile, at : at + ROWS, :] * taps[tap : tap + 1, span]
        active = mixture / (1.0 + jnp.exp(-mixture))
        encoded[:, span] = jnp.where(
            kept, attended[:, span].astype(F32) + active, 0.0
        ).astype(BF16)


def xor_pairs(count, by):
    return [(i, i ^ by) for i in range(count)]


def on_device(frames, qkv_weight, conv_kernel, lengths):
    own = frames[0]
    place_y, half = lax.axis_index("y"), lax.axis_index("zl")
    place = lax.axis_index(("zh", "x", "c"))
    sequence = half * RING + place_y
    scalars = jnp.stack([place, place_y, half, lengths[0], sequence * ROWS]).astype(jnp.int32)

    one = xor_pairs(RING, 1)
    two = [(i, (i - 1 if i % 2 == 0 else i + 1) % RING) for i in range(RING)]

    def spread(block, axis):
        copies = jnp.broadcast_to(block[None], (lax.axis_size(axis), *block.shape))
        filled = lax.all_to_all(copies, axis, split_axis=0, concat_axis=0, tiled=True)
        return filled.reshape(-1, block.shape[1])

    a1, b1 = lax.ppermute(own, "y", one), lax.ppermute(own, "y", two)
    a2, b2 = lax.ppermute(b1, "y", one), lax.ppermute(a1, "y", two)
    a3, b3 = lax.ppermute(b2, "y", one), lax.ppermute(a2, "y", two)
    a4 = lax.ppermute(b3[: ROWS // 2], "y", one)
    b4 = lax.ppermute(a3[ROWS // 2 :], "y", two)

    heads = [
        lax.dynamic_slice_in_dim(qkv_weight, (which * RING + place_y) * STRIDE, STRIDE, 1)
        for which in (half, 1 - half)
    ]
    piece = jnp.concatenate(
        heads + [conv_kernel, jnp.zeros((48, PIECE - TAPS_AT - KERNEL), BF16)], axis=1
    )
    gathered = spread(spread(piece, "zh"), "x")
    other = lax.ppermute(gathered, "c", xor_pairs(2, 1))

    edge = lax.ppermute(
        jnp.where(half == 0, own[ROWS - HALO :], own[:HALO]),
        ("zl", "y"),
        [(RING - 1, RING), (RING, RING - 1)],
    )
    even = place_y % 2 == 0
    low = jnp.where(even, b1[ROWS - HALO :], a1[ROWS - HALO :])
    high = jnp.where(even, a1[:HALO], b1[:HALO])
    low = jnp.where(place_y == 0, edge, low)
    high = jnp.where(place_y == RING - 1, edge, high)

    arrived = {0: (own,), 1: (a1,), -1: (b1,), 2: (a2,), -2: (b2,), 3: (a3,), -3: (b3,), 4: (a4, b4)}
    mine, theirs = [], []
    for index, steps in enumerate(CHUNKS):
        blocks = [block for step in steps for block in arrived[step]]
        shape = jax.ShapeDtypeStruct((len(steps) * PACKED[0], PACKED[1]), BF16)
        scratch = [pltpu.VMEM((len(steps) * ROWS, 1536), BF16)]
        if index == 0:
            full = jax.ShapeDtypeStruct((1536, PIECE), BF16)
            weight, kept, sent = call(
                first_kernel, (full, shape, shape), scalars, gathered, other, *blocks,
                scratch=scratch,
            )
        elif index == 1:
            rest = jax.ShapeDtypeStruct((32, 1536), F32)
            taps, kept, sent = call(
                second_kernel, (rest, shape, shape), scalars, weight, *blocks, scratch=scratch
            )
        else:
            kept, sent = call(
                project_kernel, (shape, shape), scalars, weight, *blocks, scratch=scratch
            )
        mine.append(kept)
        theirs.append(lax.ppermute(sent, "zl", xor_pairs(2, 1)))
    context = call(
        attention_kernel,
        jax.ShapeDtypeStruct((HEADS, GROUP_ROWS, GROUPS * HEAD_DIM), BF16),
        scalars,
        *mine,
        *theirs,
        scratch=[
            pltpu.VMEM((2 * RING * ROWS, LANES), BF16),
            pltpu.VMEM((2 * RING * ROWS, LANES), BF16),
            pltpu.VMEM((2 * RING * ROWS, LANES), BF16),
            pltpu.VMEM((2 * RING * ROWS + 2 * HALO, LANES), BF16),
        ],
    )
    returned = lax.all_to_all(context, ("zl", "y"), split_axis=0, concat_axis=0, tiled=True)
    shape = jax.ShapeDtypeStruct(own.shape, BF16)
    attended, encoded = call(
        finish_kernel,
        (shape, shape),
        scalars,
        returned,
        own,
        low,
        high,
        taps,
        scratch=[pltpu.VMEM((1536 // LANES, WINDOW, LANES), F32)],
    )
    return attended[None], encoded[None]


def solution(mesh):
    fine = Mesh(mesh.devices.reshape(4, 4, 2, 2, RING), ("zh", "x", "c", "zl", "y"))
    rows, columns = ("zh", "x", "c"), ("zl", "y")
    in_specs = (P(rows, columns, None), P(rows, None), P(rows, None), P(rows))
    out_specs = (P(rows, columns, None), P(rows, columns, None))

    return jax.shard_map(
        on_device, mesh=fine, in_specs=in_specs, out_specs=out_specs, check_vma=False
    )
```

```python
import jax
import jax.numpy as jnp
from jax import lax
from jax.experimental import pallas as pl
from jax.experimental.pallas import tpu as pltpu
from jax.sharding import Mesh
from jax.sharding import PartitionSpec as P


HEADS = 16
KERNEL = 31
HEAD_DIM = 96
EPSILON = 1e-05
NEG_BIG = -1e30

LANES = 128
ROWS = 128
RING = 8
HALO = 16
WINDOW = ROWS + 2 * HALO
GROUPS = 4
GROUP_ROWS = WINDOW // GROUPS
STRIDE = 3 * HEAD_DIM
PIECE = 640
TAPS_AT = 2 * STRIDE
PACK = 4
PACKED = (ROWS // PACK, PACK * STRIDE)
CHUNKS = ((0, 1, -1, 2, -2), (3, -3), (4,))
Q_ROWS = 256
K_ROWS = 1024

VMEM = pl.BlockSpec(memory_space=pltpu.VMEM)
SMEM = pl.BlockSpec(memory_space=pltpu.SMEM)
F32 = jnp.float32
BF16 = jnp.bfloat16


def call(kernel, outs, scalars, *arrays, scratch=()):
    return pl.pallas_call(
        kernel,
        out_shape=outs,
        in_specs=[SMEM] + [VMEM] * len(arrays),
        out_specs=jax.tree.map(lambda _: VMEM, outs),
        scratch_shapes=list(scratch),
        compiler_params=pltpu.CompilerParams(vmem_limit_bytes=16 * 2**20),
    )(scalars, *arrays)


def normalized(values):
    center = values - jnp.mean(values, axis=-1, keepdims=True)
    return center * lax.rsqrt(jnp.mean(center * center, axis=-1, keepdims=True) + EPSILON)


def project(blocks, weight, mine, theirs, normed):
    at = 0
    for block in blocks:
        rows = block.shape[0]
        normed[at : at + rows, :] = normalized(block[...].astype(F32)).astype(BF16)
        at += rows
    result = jnp.dot(normed[...], weight[...], preferred_element_type=F32)
    rows, _ = PACKED
    for block in range(at // ROWS):
        for head, target in enumerate((mine, theirs)):
            parts = []
            for group in range(PACK):
                first = block * ROWS + group * rows
                parts.append(
                    result[first : first + rows, head * STRIDE : (head + 1) * STRIDE]
                )
            target[block * rows : (block + 1) * rows, :] = jnp.concatenate(
                parts, axis=1
            ).astype(BF16)


def first_kernel(scalars, own, other, *refs):
    *blocks, weight, mine, theirs, normed = refs
    core = scalars[0] % 2
    rows = 48
    for source, which in ((own, core), (other, 1 - core)):
        for x in range(4):
            for z in range(4):
                target = pl.multiple_of((z * 8 + x * 2 + which) * rows, 16)
                at = (x * 4 + z) * rows
                weight[pl.ds(target, rows), :] = source[at : at + rows, :]
    project(blocks, weight, mine, theirs, normed)


def second_kernel(scalars, weight, *refs):
    *blocks, taps, mine, theirs, normed = refs
    first = TAPS_AT - (PIECE - LANES)
    for tile in range(1536 // LANES):
        span = slice(tile * LANES, (tile + 1) * LANES)
        taps[:, span] = weight[span, PIECE - LANES :].astype(F32).T[first : first + 32, :]
    project(blocks, weight, mine, theirs, normed)


def project_kernel(scalars, weight, *refs):
    *blocks, mine, theirs, normed = refs
    project(blocks, weight, mine, theirs, normed)


def attention_kernel(scalars, *refs):
    groups = len(CHUNKS)
    chunks, out = refs[: 2 * groups], refs[2 * groups]
    queries, keys, values, context, turned_values, table, tops = refs[2 * groups + 1 :]
    y, half, length = scalars[1], scalars[2], scalars[3]
    sign = 1 - 2 * (y % 2)
    rows = ROWS // PACK
    row = lax.broadcasted_iota(jnp.int32, (rows, LANES), 0)
    blank = jnp.zeros((rows, LANES - HEAD_DIM), F32)
    marked = lax.broadcasted_iota(jnp.int32, (rows, LANES), 1) == HEAD_DIM
    for side in range(2):
        for group, steps in enumerate(CHUNKS):
            chunk = chunks[side * groups + group]
            for index, step in enumerate(steps):
                source = (y + sign * step + RING) % RING
                which = half if side == 0 else 1 - half
                packed = chunk[index * rows : (index + 1) * rows, :].astype(F32)
                for part in range(PACK):
                    start = (which * RING + source) * ROWS + part * rows
                    to = pl.ds(pl.multiple_of(start, rows), rows)
                    ends = (1.0, jnp.where(start + row < length, 0.0, NEG_BIG), 1.0)
                    for kind, target in enumerate((queries, keys, values)):
                        first = part * STRIDE + kind * HEAD_DIM
                        columns = packed[:, first : first + HEAD_DIM]
                        columns = jnp.concatenate([columns, blank], axis=1)
                        target[to, :] = jnp.where(marked, ends[kind], columns).astype(BF16)
    total = queries.shape[0]
    factor = HEAD_DIM**-0.5 * 1.4426950408889634
    context[:HALO, :] = jnp.zeros((HALO, LANES), BF16)
    context[HALO + total :, :] = jnp.zeros((HALO, LANES), BF16)

    turned_values[...] = values[...].astype(F32).T.astype(BF16)
    steps = total // Q_ROWS
    parts = [slice(b * K_ROWS, (b + 1) * K_ROWS) for b in range(total // K_ROWS)]

    def score(index, part):
        query = queries[pl.ds(pl.multiple_of(index * Q_ROWS, Q_ROWS), Q_ROWS), :]
        return lax.dot_general(
            keys[part, :], query, (((1,), (1,)), ((), ())), preferred_element_type=F32
        )

    def both(index, now, after):
        highest = tops[now : now + 1, :]
        raised = None
        summed = jnp.zeros((LANES, Q_ROWS), F32)
        following = jnp.minimum(index + 1, steps - 1)
        for part in parts:
            block = score(following, part)
            table[after, part, :] = block
            top = jnp.max(block, axis=0, keepdims=True)
            raised = top if raised is None else jnp.maximum(raised, top)
            weights = jnp.exp2((table[now, part, :] - highest) * factor).astype(BF16)
            summed += jnp.dot(turned_values[:, part], weights, preferred_element_type=F32)
        tops[after : after + 1, :] = raised
        result = summed / summed[HEAD_DIM : HEAD_DIM + 1, :]
        first = pl.multiple_of(index * Q_ROWS, Q_ROWS)
        context[pl.ds(HALO + first, Q_ROWS), :] = result.T.astype(BF16)

    raised = None
    for part in parts:
        block = score(0, part)
        table[0, part, :] = block
        top = jnp.max(block, axis=0, keepdims=True)
        raised = top if raised is None else jnp.maximum(raised, top)
    tops[0:1, :] = raised

    def visit(index, _):
        both(2 * index, 0, 1)
        both(2 * index + 1, 1, 0)
        return 0

    lax.fori_loop(0, steps // 2, visit, 0)
    for target in range(total // ROWS):
        parts = [
            context[
                target * ROWS + group * GROUP_ROWS : target * ROWS + (group + 1) * GROUP_ROWS,
                :HEAD_DIM,
            ]
            for group in range(GROUPS)
        ]
        out[target] = jnp.concatenate(parts, axis=1)


def finish_kernel(scalars, returned, own, low, high, taps, attended, encoded, wide):
    begin, length = scalars[4], scalars[3]
    rows = []
    for group in range(GROUPS):
        span = slice(group * HEAD_DIM, (group + 1) * HEAD_DIM)
        rows.append(
            jnp.concatenate([returned[head, :, span] for head in range(HEADS)], axis=1)
        )
    context = jnp.concatenate(rows, axis=0).astype(F32)
    inputs = jnp.concatenate([low[...], own[...], high[...]], axis=0).astype(F32)
    position = begin - HALO + lax.broadcasted_iota(jnp.int32, (WINDOW, 1), 0)
    valid = jnp.logical_and(position >= 0, position < length)
    summed = jnp.where(valid, inputs + context, 0.0).astype(BF16)
    attended[...] = summed[HALO : HALO + ROWS, :]
    conv_input = jnp.where(valid, normalized(summed.astype(F32)), 0.0).astype(BF16).astype(F32)
    tiles = wide.shape[0]
    for tile in range(tiles):
        wide[tile] = conv_input[:, tile * LANES : (tile + 1) * LANES]
    kept = valid[HALO : HALO + ROWS]
    for tile in range(tiles):
        span = slice(tile * LANES, (tile + 1) * LANES)
        mixture = jnp.zeros((ROWS, LANES), F32)
        for tap in range(KERNEL):
            at = tap + HALO - KERNEL // 2
            mixture = mixture + wide[tile, at : at + ROWS, :] * taps[tap : tap + 1, span]
        active = mixture / (1.0 + jnp.exp(-mixture))
        encoded[:, span] = jnp.where(
            kept, attended[:, span].astype(F32) + active, 0.0
        ).astype(BF16)


def xor_pairs(count, by):
    return [(i, i ^ by) for i in range(count)]


def on_device(frames, qkv_weight, conv_kernel, lengths):
    own = frames[0]
    place_y, half = lax.axis_index("y"), lax.axis_index("zl")
    place = lax.axis_index(("zh", "x", "c"))
    sequence = half * RING + place_y
    scalars = jnp.stack([place, place_y, half, lengths[0], sequence * ROWS]).astype(jnp.int32)

    one = xor_pairs(RING, 1)
    two = [(i, (i - 1 if i % 2 == 0 else i + 1) % RING) for i in range(RING)]

    def spread(block, axis):
        copies = jnp.broadcast_to(block[None], (lax.axis_size(axis), *block.shape))
        filled = lax.all_to_all(copies, axis, split_axis=0, concat_axis=0, tiled=True)
        return filled.reshape(-1, block.shape[1])

    a1, b1 = lax.ppermute(own, "y", one), lax.ppermute(own, "y", two)
    a2, b2 = lax.ppermute(b1, "y", one), lax.ppermute(a1, "y", two)
    a3, b3 = lax.ppermute(b2, "y", one), lax.ppermute(a2, "y", two)
    a4 = lax.ppermute(b3[: ROWS // 2], "y", one)
    b4 = lax.ppermute(a3[ROWS // 2 :], "y", two)

    heads = [
        lax.dynamic_slice_in_dim(qkv_weight, (which * RING + place_y) * STRIDE, STRIDE, 1)
        for which in (half, 1 - half)
    ]
    piece = jnp.concatenate(
        heads + [conv_kernel, jnp.zeros((48, PIECE - TAPS_AT - KERNEL), BF16)], axis=1
    )
    gathered = spread(spread(piece, "zh"), "x")
    other = lax.ppermute(gathered, "c", xor_pairs(2, 1))

    edge = lax.ppermute(
        jnp.where(half == 0, own[ROWS - HALO :], own[:HALO]),
        ("zl", "y"),
        [(RING - 1, RING), (RING, RING - 1)],
    )
    even = place_y % 2 == 0
    low = jnp.where(even, b1[ROWS - HALO :], a1[ROWS - HALO :])
    high = jnp.where(even, a1[:HALO], b1[:HALO])
    low = jnp.where(place_y == 0, edge, low)
    high = jnp.where(place_y == RING - 1, edge, high)

    arrived = {0: (own,), 1: (a1,), -1: (b1,), 2: (a2,), -2: (b2,), 3: (a3,), -3: (b3,), 4: (a4, b4)}
    mine, theirs = [], []
    for index, steps in enumerate(CHUNKS):
        blocks = [block for step in steps for block in arrived[step]]
        shape = jax.ShapeDtypeStruct((len(steps) * PACKED[0], PACKED[1]), BF16)
        scratch = [pltpu.VMEM((len(steps) * ROWS, 1536), BF16)]
        if index == 0:
            full = jax.ShapeDtypeStruct((1536, PIECE), BF16)
            weight, kept, sent = call(
                first_kernel, (full, shape, shape), scalars, gathered, other, *blocks,
                scratch=scratch,
            )
        elif index == 1:
            rest = jax.ShapeDtypeStruct((32, 1536), F32)
            taps, kept, sent = call(
                second_kernel, (rest, shape, shape), scalars, weight, *blocks, scratch=scratch
            )
        else:
            kept, sent = call(
                project_kernel, (shape, shape), scalars, weight, *blocks, scratch=scratch
            )
        mine.append(kept)
        theirs.append(lax.ppermute(sent, "zl", xor_pairs(2, 1)))
    context = call(
        attention_kernel,
        jax.ShapeDtypeStruct((HEADS, GROUP_ROWS, GROUPS * HEAD_DIM), BF16),
        scalars,
        *mine,
        *theirs,
        scratch=[
            pltpu.VMEM((2 * RING * ROWS, LANES), BF16),
            pltpu.VMEM((2 * RING * ROWS, LANES), BF16),
            pltpu.VMEM((2 * RING * ROWS, LANES), BF16),
            pltpu.VMEM((2 * RING * ROWS + 2 * HALO, LANES), BF16),
            pltpu.VMEM((LANES, 2 * RING * ROWS), BF16),
            pltpu.VMEM((2, 2 * RING * ROWS, Q_ROWS), F32),
            pltpu.VMEM((8, Q_ROWS), F32),
        ],
    )
    returned = lax.all_to_all(context, ("zl", "y"), split_axis=0, concat_axis=0, tiled=True)
    shape = jax.ShapeDtypeStruct(own.shape, BF16)
    attended, encoded = call(
        finish_kernel,
        (shape, shape),
        scalars,
        returned,
        own,
        low,
        high,
        taps,
        scratch=[pltpu.VMEM((1536 // LANES, WINDOW, LANES), F32)],
    )
    return attended[None], encoded[None]


def solution(mesh):
    fine = Mesh(mesh.devices.reshape(4, 4, 2, 2, RING), ("zh", "x", "c", "zl", "y"))
    rows, columns = ("zh", "x", "c"), ("zl", "y")
    in_specs = (P(rows, columns, None), P(rows, None), P(rows, None), P(rows))
    out_specs = (P(rows, columns, None), P(rows, columns, None))

    return jax.shard_map(
        on_device, mesh=fine, in_specs=in_specs, out_specs=out_specs, check_vma=False
    )
```
